128 devices in a mesh: row: 8 (over z_lo, y), col: 16 (over x, z_hi, core).
Axes of the slice: x: 4, y: 4, z: 4 (z_hi: 2, z_lo: 2; z = z_hi * 2 + z_lo), core: 2. Of those that a mesh axis runs over, the one named last changes fastest.
Arguments:
- panel: bfloat16 [524288, 256], P(('row', 'col')), may hold values from -6 to 6
- row_basis: bfloat16 [524288, 16], P('row'), may hold values from -1.5 to 1.5
- col_basis: bfloat16 [524288, 16], P(('row', 'col')), may hold values from -0.375 to 0.375
- near_blocks: bfloat16 [2048, 9, 256, 256], P(('row', 'col')), may hold values from -0.125 to 0.125
- couplings: bfloat16 [8, 16, 512, 16, 16], P('row', 'col'), may hold values from -0.375 to 0.375
- blk_rows: int32 [8, 16, 512], P('row', 'col'), may hold values from 0 to 255
- blk_cols: int32 [8, 16, 512], P('row', 'col'), may hold values from 0 to 127
- blk_count: int32 [8, 16], P('row', 'col'), may hold values from 64 to 512, as said below
Outputs:
- product: bfloat16 [524288, 256], P(('row', 'col'))
The draws below stay inside these ranges and needn't reach their ends.
Inputs may be any that keep to these rules, and one draw needn't show every extreme that they name: `blk_count`: slots at or past a device's count hold in-range indices and are not part of the matrix; in every draw some device holds 512 live slots.
All inputs are finite; a program needn't handle non-finite values.
Results may differ from the reference program's by a relative error of at most 0.0052.
Values may be sent and summed in bfloat16 or wider, within the bound.
A program may use at most 192 MiB of HBM per device.

```python
import jax
import jax.numpy as jnp
from jax import lax

LEAF = 256
R = 16
NRHS = 256
HALF = 4
FAR_PER_CL = 32
CPD = 16
NEAR = 9
FAR_DEV = 512
NCL = 2048
NPTS = 524288
N_ROW = 8
N_COL = 16


def draw_blk_count(key, part):
    first_key, second_key = jax.random.split(jax.random.fold_in(key, 17))
    raw_level = jax.random.randint(first_key, (N_ROW * N_COL,), 0, 64)
    lowest = FAR_DEV // 8
    counts = lowest + (FAR_DEV - lowest) * raw_level * raw_level // (63 * 63)
    fullest = jax.random.randint(second_key, (), 0, N_ROW * N_COL)
    counts = jnp.where(jnp.arange(N_ROW * N_COL) == fullest, FAR_DEV, counts)
    return counts.reshape(N_ROW, N_COL).astype(jnp.int32)


def set_ends(entries, key, low, largest):
    extent = entries.shape
    spot = [jax.random.randint(jax.random.fold_in(key, axis), (), 0, extent[axis]) for axis in range(len(extent))]
    entries = entries.at[tuple(spot)].set(low)
    longest = extent.index(max(extent))
    spot[longest] = (spot[longest] + 1) % extent[longest]
    return entries.at[tuple(spot)].set(largest)


def block_scale(rng, shape, shards, low, top_value):
    factor_of, own = 1.0, jax.random.fold_in(rng, 6)
    for axis_at, parts in shards:
        heights = jnp.exp(jax.random.uniform(jax.random.fold_in(own, axis_at), (parts,), jnp.float32, low / len(shards), top_value / len(shards)))
        factor_of = factor_of * jnp.repeat(heights, shape[axis_at] // parts).reshape([-1 if axis == axis_at else 1 for axis in range(len(shape))])
    return factor_of


def gaussian(key, shape, width, bound, pieces=(), held_as=jnp.bfloat16):
    values = jax.random.normal(key, shape, jnp.float32) * width
    if len(pieces) > 0:
        values = block_scale(key, shape, pieces, -0.22, 0.18) * values
    return jnp.clip(values, min=-bound, max=bound).astype(held_as)


def setup_inputs(seed: int = 0) -> dict:
    seeds = jax.random.split(jax.random.key(seed), 9)
    return {
        "panel": gaussian(seeds[0], (NPTS, NRHS), 1.0, 6.0, ((0, 128),)),
        "row_basis": gaussian(seeds[1], (NPTS, R), R ** -0.5, 1.5, ((0, 8),)),
        "col_basis": gaussian(seeds[2], (NPTS, R), LEAF ** -0.5, 0.375, ((0, 128),)),
        "near_blocks": gaussian(seeds[3], (NCL, NEAR, LEAF, LEAF), (NEAR * LEAF) ** -0.5, 0.125, ((0, 128),)),
        "couplings": gaussian(seeds[4], (N_ROW, N_COL, FAR_DEV, R, R), (R * FAR_PER_CL // 2) ** -0.5, 0.375, ((0, 8), (1, 16))),
        "blk_rows": set_ends(jax.random.randint(seeds[5], (N_ROW, N_COL, FAR_DEV), 0, N_COL * CPD), jax.random.fold_in(seeds[5], 1), 0, (N_COL * CPD) - 1).astype(jnp.int32),
        "blk_cols": set_ends(jax.random.randint(seeds[6], (N_ROW, N_COL, FAR_DEV), 0, N_ROW * CPD), jax.random.fold_in(seeds[6], 1), 0, (N_ROW * CPD) - 1).astype(jnp.int32),
        "blk_count": draw_blk_count(jax.random.fold_in(seeds[8], 71), 0),
    }


def reference(panel, row_basis, col_basis, near_blocks, couplings, blk_rows, blk_cols, blk_count):
    cluster_total = NPTS // LEAF
    highest = lax.Precision.HIGHEST
    clusters = panel.reshape(cluster_total, LEAF, NRHS).astype(jnp.float32)
    coeffs = jnp.einsum('kpr,kpn->krn', col_basis.reshape(cluster_total, LEAF, R).astype(jnp.float32), clusters, precision=highest).astype(jnp.bfloat16)
    owner_row = jnp.arange(N_ROW, dtype=jnp.int32)[:, None, None]
    owner_col = jnp.arange(N_COL, dtype=jnp.int32)[None, :, None]
    global_row = owner_row * (N_COL * CPD) + blk_rows
    global_col = ((blk_cols // CPD) * N_COL + owner_col) * CPD + blk_cols % CPD
    is_live = jnp.arange(FAR_DEV, dtype=jnp.int32)[None, None, :] < blk_count[:, :, None]
    slot_total = N_ROW * N_COL * FAR_DEV
    picked = coeffs[global_col.reshape(slot_total)].astype(jnp.float32)
    block_terms = jnp.einsum('bij,bjn->bin', couplings.reshape(slot_total, R, R).astype(jnp.float32), picked, precision=highest)
    block_terms = jnp.where(is_live.reshape(slot_total)[:, None, None], block_terms, jnp.float32(0.0))
    coupled = jax.ops.segment_sum(block_terms, global_row.reshape(slot_total), num_segments=cluster_total)
    far_field = jnp.einsum('kpr,krn->kpn', row_basis.reshape(cluster_total, LEAF, R).astype(jnp.float32), coupled, precision=highest)
    padded = jnp.pad(clusters, ((HALF, HALF), (0, 0), (0, 0)))
    near_field = jnp.zeros((cluster_total, LEAF, NRHS), jnp.float32)
    for offset in range(NEAR):
        near_field = near_field + jnp.einsum('kpq,kqn->kpn', near_blocks[:, offset].astype(jnp.float32), padded[offset:offset + cluster_total], precision=highest)
    return (near_field + far_field).reshape(NPTS, NRHS).astype(jnp.bfloat16)
```

```python
import functools

import jax
import jax.numpy as jnp
from jax import lax
from jax.experimental import pallas as pl
from jax.experimental.pallas import tpu as pltpu
from jax.sharding import PartitionSpec as P

MESH = pl.DeviceIdType.MESH
F32 = jnp.float32
BF16 = jnp.bfloat16

LEAF = 256
R = 16
N = 256
K = 16
HALF = 4
NEAR = 9
SLOTS = 512
GROUPS = SLOTS // 16
ROWCL = 256


def mm(a, b):
    return jnp.dot(a, b, preferred_element_type=F32)


def mm_t(a, b):
    return lax.dot_general(a, b, (((0,), (0,)), ((), ())), preferred_element_type=F32)


def iota(shape, dim):
    return lax.broadcasted_iota(jnp.int32, shape, dim)


def kernel(
    panel_hbm, ut_hbm, vt_hbm, near_hbm, ct_hbm, rows_ref, cols_ref, cnt_ref,
    out_hbm,
    pext, vt, ut, ct, nb, nat, call, expand, lmat, xmat, tmat, ohc, ohr, uexp,
    pp, po, r0, qs, r1, r2, zs, r3, cpl, nearv, outv,
    lsem, nsem, osem, ssem, rsem,
):
    row = lax.axis_index("row")
    col = lax.axis_index("col")
    zl, y = row // 4, row % 4
    x, zh, core = col // 4, (col // 2) % 2, col % 2

    def at(zl_, y_, x_, zh_, core_):
        return (zl_ * 4 + y_, x_ * 4 + zh_ * 2 + core_)

    yp, ym = (y + 1) % 4, (y + 3) % 4
    xp, xm = (x + 1) % 4, (x + 3) % 4
    d_core = at(zl, y, x, zh, 1 - core)
    d_xp, d_xm = at(zl, y, xp, zh, core), at(zl, y, xm, zh, core)
    d_yp, d_ym = at(zl, yp, x, zh, core), at(zl, ym, x, zh, core)
    d_zl = at(1 - zl, y, x, zh, core)
    d_zh = at(zl, y, x, 1 - zh, core)
    lin = row * 16 + col
    has_l, has_r = lin > 0, lin < 127
    left, right = jnp.maximum(lin - 1, 0), jnp.minimum(lin + 1, 127)
    d_left, d_right = (left // 16, left % 16), (right // 16, right % 16)

    own = pl.ds(HALF * LEAF, K * LEAF)
    c_panel = pltpu.make_async_copy(panel_hbm, pext.at[own], lsem.at[0])
    c_vt = pltpu.make_async_copy(vt_hbm, vt, lsem.at[1])
    c_ct = pltpu.make_async_copy(ct_hbm, ct, lsem.at[2])
    c_ut = pltpu.make_async_copy(
        ut_hbm.at[:, pl.ds(pl.multiple_of(col * (K * LEAF), K * LEAF), K * LEAF)], ut, lsem.at[3]
    )
    c_panel.start()
    c_vt.start()

    barrier = pltpu.get_barrier_semaphore()
    for dev in (d_core, d_xp, d_xm, d_yp, d_ym, d_zl, d_zh):
        pl.semaphore_signal(barrier, inc=1, device_id=dev, device_id_type=MESH)

    @pl.when(has_l)
    def _():
        pl.semaphore_signal(barrier, inc=1, device_id=d_left, device_id_type=MESH)

    @pl.when(has_r)
    def _():
        pl.semaphore_signal(barrier, inc=1, device_id=d_right, device_id_type=MESH)

    c_ct.start()
    c_ut.start()

    def near_copy(k):
        return pltpu.make_async_copy(near_hbm.at[k], nb.at[k], nsem.at[k])

    near_order = list(range(4, 12)) + [3, 2, 1, 0] + list(range(12, 16))
    for k in near_order:
        near_copy(k).start()

    a256, b256 = iota((256, 256), 0), iota((256, 256), 1)
    perm = jnp.where((b256 // 16 == a256 % 16) & (b256 % 16 == a256 // 16), 1.0, 0.0).astype(BF16)
    e_mat = jnp.where(iota((R, 256), 1) // 16 == iota((R, 256), 0), 1.0, 0.0).astype(BF16)
    expand[...] = e_mat
    c_panel.wait()
    c_vt.wait()
    for k in range(K):
        nat[k * R:(k + 1) * R, :] = mm(
            vt[:, k * LEAF:(k + 1) * LEAF], pext[(HALF + k) * LEAF:(HALF + k + 1) * LEAF, :]
        ).astype(BF16)
    call[row] = mm(perm, nat[...]).astype(BF16).reshape(R, K, N)

    pl.semaphore_wait(barrier, 7 + has_l.astype(jnp.int32) + has_r.astype(jnp.int32))

    def rc(m, src, dst, dev):
        return pltpu.make_async_remote_copy(
            src_ref=src, dst_ref=dst, send_sem=ssem.at[m], recv_sem=rsem.at[m],
            device_id=dev, device_id_type=MESH,
        )

    def piece(m, slot, half, dev):
        ref = call.at[slot, pl.ds(half * 8, 8)]
        return rc(m, ref, ref, dev)

    s_zp = (1 - zl) * 4 + y
    s_ym, s_yp = zl * 4 + ym, zl * 4 + yp
    sz_ym, sz_yp = (1 - zl) * 4 + ym, (1 - zl) * 4 + yp
    ga = {
        0: piece(0, row, 0, d_zl), 1: piece(1, row, 1, d_zl),
        2: piece(2, row, 0, d_yp), 3: piece(3, row, 1, d_yp),
        4: piece(4, row, 0, d_ym), 5: piece(5, row, 1, d_ym),
        6: piece(6, s_zp, 0, d_yp), 7: piece(7, s_zp, 1, d_yp),
        8: piece(8, s_zp, 0, d_ym), 9: piece(9, s_zp, 1, d_ym),
        10: piece(10, s_ym, 0, d_yp), 11: piece(11, s_yp, 1, d_ym),
        12: piece(12, sz_ym, 0, d_yp), 13: piece(13, sz_yp, 1, d_ym),
    }
    for m in (0, 1, 2, 5, 3, 4):
        ga[m].start()

    tail = pl.ds(K * LEAF, HALF * LEAF)
    head = pl.ds(HALF * LEAF, HALF * LEAF)
    lo = pl.ds(0, HALF * LEAF)
    hi = pl.ds((HALF + K) * LEAF, HALF * LEAF)
    h_right = rc(30, pext.at[tail], pext.at[lo], d_right)
    h_left = rc(31, pext.at[head], pext.at[hi], d_left)

    @pl.when(has_r)
    def _():
        h_right.start()

    @pl.when(has_l)
    def _():
        h_left.start()

    c_ct.wait()

    def l_body(i, carry):
        v = mm_t(ct[i], expand[...])
        keep = iota((SLOTS, 256), 0) % 16 == iota((SLOTS, 256), 1) % 16
        lmat[:, i] = jnp.where(keep, v, 0.0).astype(BF16).reshape(GROUPS, 16, 256)
        return carry

    lax.fori_loop(0, R, l_body, 0)

    ga[2].wait_recv()
    ga[10].start()
    ga[5].wait_recv()
    ga[11].start()

    c_ut.wait()

    def u_body(k, carry):
        cols = pl.ds(pl.multiple_of(k * LEAF, LEAF), LEAF)
        v = mm_t(ut[:, cols], expand[...])
        keep = iota((LEAF, 256), 1) % 16 == k
        uexp[pl.ds(pl.multiple_of(k * LEAF, LEAF), LEAF), :] = jnp.where(keep, v, 0.0).astype(BF16)
        return carry

    lax.fori_loop(0, K, u_body, 0)

    ga[0].wait_recv()
    ga[6].start()
    ga[8].start()
    ga[1].wait_recv()
    ga[9].start()
    ga[7].start()

    oct_ = jnp.where(iota((128, SLOTS), 0) == cols_ref[...], 1.0, 0.0).astype(F32)
    ohc[...] = oct_.T.astype(BF16)
    ra = iota((ROWCL, SLOTS), 0)
    kk, dz, pos, dc = ra % 16, 1 - (ra // 16) % 2, (ra // 32) % 4, 1 - ra // 128
    dx = jnp.where(pos == 0, 2, jnp.where(pos == 1, 1, jnp.where(pos == 2, 3, 0)))
    cluster = (((x + dx) % 4) * 4 + ((zh + dz) % 2) * 2 + (core + dc) % 2) * 16 + kk
    live = iota((ROWCL, SLOTS), 1) < cnt_ref[0, 0]
    ohr[...] = jnp.where((cluster == rows_ref[...]) & live, 1.0, 0.0).astype(BF16)

    def near_row(k):
        acc = mm(nb[k, 0], pext[pl.ds(pl.multiple_of(k * LEAF, LEAF), LEAF), :])
        for o in range(1, NEAR):
            acc += mm(nb[k, o], pext[pl.ds(pl.multiple_of((k + o) * LEAF, LEAF), LEAF), :])
        nearv[k] = acc

    def near_rows(start, stop):
        def body(k, carry):
            near_copy(k).wait()
            near_row(k)
            return carry
        lax.fori_loop(start, stop, body, 0)

    near_rows(4, 8)
    ga[6].wait_recv()
    ga[12].start()
    ga[9].wait_recv()
    ga[13].start()
    near_rows(8, 12)
    for m in (3, 4, 10, 11, 7, 8, 12, 13):
        ga[m].wait_recv()

    def x_body(j, carry):
        cj = call[:, j].reshape(128, N)
        xmat[:, j] = mm(ohc[...], cj).astype(BF16).reshape(GROUPS, 16, N)
        return carry

    lax.fori_loop(0, R, x_body, 0)

    def t_body(g, carry):
        t = mm(lmat[g].reshape(256, 256), xmat[g].reshape(256, N))
        tmat[:, g] = t.astype(BF16).reshape(R, 16, N)
        return carry

    lax.fori_loop(0, GROUPS, t_body, 0)

    core_send = [rc(14 + h, pp.at[h], r0.at[h], d_core) for h in range(2)]
    for h in range(2):
        def p_body(i, carry, h=h):
            p = mm(ohr[...], tmat[h * 8 + i].reshape(SLOTS, N))
            pp[h, :, :, i] = p[:128].astype(BF16).reshape(4, 2, 16, N)
            po[h, :, :, i] = p[128:].reshape(4, 2, 16, N)
            return carry

        lax.fori_loop(0, 8, p_body, 0)
        core_send[h].start()

    b1p = [rc(16 + h, qs.at[h, 0, 0], r1.at[h, 0], d_xp) for h in range(2)]
    b1m = [rc(18 + h, qs.at[h, 0, 1], r1.at[h, 1], d_xm) for h in range(2)]
    b2p0 = [rc(20 + h, qs.at[h, 1, 1], r2.at[h, 0, 1], d_xp) for h in range(2)]
    b2m1 = [rc(22 + h, qs.at[h, 2, 0], r2.at[h, 1, 0], d_xm) for h in range(2)]
    b2p1 = [rc(24 + h, qs.at[h, 1, 0], r2.at[h, 0, 0], d_xp) for h in range(2)]
    b2m0 = [rc(26 + h, qs.at[h, 2, 1], r2.at[h, 1, 1], d_xm) for h in range(2)]
    bz = [rc(28 + h, zs.at[h], r3.at[h], d_zh) for h in range(2)]

    def fold(h, pos, dzi):
        return po[h, pos, dzi] + r0[h, pos, dzi].astype(F32)

    for h in range(2):
        core_send[h].wait_recv()
        qs[h, 0, 0] = fold(h, 0, 0).astype(BF16)
        qs[h, 0, 1] = fold(h, 0, 1).astype(BF16)
        b1p[h].start()
        b1m[h].start()
        qs[h, 1, 1] = fold(h, 1, 1).astype(BF16)
        qs[h, 2, 0] = fold(h, 2, 0).astype(BF16)
        b2p0[h].start()
        b2m1[h].start()

    @pl.when(has_l)
    def _():
        h_right.wait_recv()

    @pl.when(jnp.logical_not(has_l))
    def _():
        pext[lo] = jnp.zeros((HALF * LEAF, N), BF16)

    near_rows(0, 2)
    for h in range(2):
        b1p[h].wait_recv()
        qs[h, 1, 0] = (fold(h, 1, 0) + r1[h, 0].astype(F32)).astype(BF16)
        b2p1[h].start()
        b1m[h].wait_recv()
        qs[h, 2, 1] = (fold(h, 2, 1) + r1[h, 1].astype(F32)).astype(BF16)
        b2m0[h].start()

    near_rows(2, 4)

    @pl.when(has_r)
    def _():
        h_left.wait_recv()

    @pl.when(jnp.logical_not(has_r))
    def _():
        pext[hi] = jnp.zeros((HALF * LEAF, N), BF16)

    near_rows(12, 16)

    for h in range(2):
        b2p1[h].wait_recv()
        b2m1[h].wait_recv()
        zs[h] = (fold(h, 3, 0) + r2[h, 0, 0].astype(F32) + r2[h, 1, 0].astype(F32)).astype(BF16)
        bz[h].start()
    for h in range(2):
        b2p0[h].wait_recv()
        b2m0[h].wait_recv()
        po[h, 3, 1] = fold(h, 3, 1) + r2[h, 0, 1].astype(F32) + r2[h, 1, 1].astype(F32)
    for h in range(2):
        bz[h].wait_recv()
        cpl[pl.ds(h * 8, 8)] = (po[h, 3, 1] + r3[h].astype(F32)).astype(BF16)

    def out_copy(k):
        return pltpu.make_async_copy(
            outv.at[k], out_hbm.at[pl.ds(pl.multiple_of(k * LEAF, LEAF), LEAF)], osem.at[k]
        )

    def o_body(k, carry):
        far = mm(uexp[pl.ds(pl.multiple_of(k * LEAF, LEAF), LEAF), :], cpl[...].reshape(256, N))
        outv[k] = (nearv[k] + far).astype(BF16)
        out_copy(k).start()
        return carry

    lax.fori_loop(0, K, o_body, 0)

    for m in range(14):
        ga[m].wait_send()
    for group in (core_send, b1p, b1m, b2p0, b2m1, b2p1, b2m0, bz):
        for copy in group:
            copy.wait_send()

    @pl.when(has_r)
    def _():
        h_right.wait_send()

    @pl.when(has_l)
    def _():
        h_left.wait_send()

    def w_body(k, carry):
        out_copy(k).wait()
        return carry

    lax.fori_loop(0, K, w_body, 0)


def on_device(panel, row_basis, col_basis, near_blocks, couplings, blk_rows, blk_cols, blk_count):
    any_ = pl.BlockSpec(memory_space=pl.ANY)
    vm = pl.BlockSpec(memory_space=pltpu.VMEM)
    sm = pl.BlockSpec(memory_space=pltpu.SMEM)
    scratch = [
        pltpu.VMEM(((K + 2 * HALF) * LEAF, N), BF16),
        pltpu.VMEM((R, K * LEAF), BF16),
        pltpu.VMEM((R, K * LEAF), BF16),
        pltpu.VMEM((R, R, SLOTS), BF16),
        pltpu.VMEM((K, NEAR, LEAF, LEAF), BF16),
        pltpu.VMEM((K * R, N), BF16),
        pltpu.VMEM((8, R, K, N), BF16),
        pltpu.VMEM((R, 256), BF16),
        pltpu.VMEM((GROUPS, R, 16, 256), BF16),
        pltpu.VMEM((GROUPS, R, 16, N), BF16),
        pltpu.VMEM((R, GROUPS, 16, N), BF16),
        pltpu.VMEM((SLOTS, 128), BF16),
        pltpu.VMEM((ROWCL, SLOTS), BF16),
        pltpu.VMEM((K * LEAF, 256), BF16),
        pltpu.VMEM((2, 4, 2, 8, 16, N), BF16),
        pltpu.VMEM((2, 4, 2, 8, 16, N), F32),
        pltpu.VMEM((2, 4, 2, 8, 16, N), BF16),
        pltpu.VMEM((2, 3, 2, 8, 16, N), BF16),
        pltpu.VMEM((2, 2, 8, 16, N), BF16),
        pltpu.VMEM((2, 2, 2, 8, 16, N), BF16),
        pltpu.VMEM((2, 8, 16, N), BF16),
        pltpu.VMEM((2, 8, 16, N), BF16),
        pltpu.VMEM((R, K, N), BF16),
        pltpu.VMEM((K, LEAF, N), F32),
        pltpu.VMEM((K, LEAF, N), BF16),
        pltpu.SemaphoreType.DMA((4,)),
        pltpu.SemaphoreType.DMA((K,)),
        pltpu.SemaphoreType.DMA((K,)),
        pltpu.SemaphoreType.DMA((32,)),
        pltpu.SemaphoreType.DMA((32,)),
    ]
    return pl.pallas_call(
        kernel,
        out_shape=jax.ShapeDtypeStruct((K * LEAF, N), BF16),
        in_specs=[any_, any_, any_, any_, any_, vm, vm, sm],
        out_specs=any_,
        scratch_shapes=scratch,
        compiler_params=pltpu.CompilerParams(
            collective_id=0, has_side_effects=True, vmem_limit_bytes=66_000_000
        ),
    )(
        panel,
        row_basis.T,
        col_basis.T,
        near_blocks,
        couplings.reshape(SLOTS, R, R).transpose(1, 2, 0),
        blk_rows.reshape(1, SLOTS),
        blk_cols.reshape(1, SLOTS),
        blk_count,
    )


def solution(mesh):
    placed = (
        P(("row", "col"), None),
        P("row", None),
        P(("row", "col"), None),
        P(("row", "col"), None, None, None),
        P("row", "col", None, None, None),
        P("row", "col", None),
        P("row", "col", None),
        P("row", "col"),
    )
    return jax.shard_map(
        on_device, mesh=mesh, in_specs=placed, out_specs=P(("row", "col"), None), check_vma=False
    )
```

```python
import jax
import jax.numpy as jnp
from jax import lax
from jax.experimental import pallas as pl
from jax.experimental.pallas import tpu as pltpu
from jax.sharding import PartitionSpec as P

MESH = pl.DeviceIdType.MESH
F32 = jnp.float32
BF16 = jnp.bfloat16

LEAF = 256
R = 16
N = 256
HN = N // 2
K = 16
HALF = 4
NEAR = 9
SLOTS = 512
GROUPS = SLOTS // 16
ROWCL = 256


def mm(a, b):
    return jnp.dot(a, b, preferred_element_type=F32)


def mm_t(a, b):
    return lax.dot_general(a, b, (((0,), (0,)), ((), ())), preferred_element_type=F32)


def iota(shape, dim):
    return lax.broadcasted_iota(jnp.int32, shape, dim)


def kernel(
    panel_hbm, ut_hbm, vt_hbm, near_hbm, ct_hbm, rows_ref, cols_ref, cnt_ref,
    out_ref,
    pext, vt, ut, utt, ct, nb, call0, call1, expand, perm, lmat, tmat, ohr,
    pp, po, r0, qs, r1, r2, zs, r3, cplk, nearv,
    lsem, nsem, ssem, rsem,
):
    row = lax.axis_index("row")
    col = lax.axis_index("col")
    zl, y = row // 4, row % 4
    x, zh, core = col // 4, (col // 2) % 2, col % 2

    def at(zl_, y_, x_, zh_, core_):
        return (zl_ * 4 + y_, x_ * 4 + zh_ * 2 + core_)

    yp, ym = (y + 1) % 4, (y + 3) % 4
    xp, xm = (x + 1) % 4, (x + 3) % 4
    d_core = at(zl, y, x, zh, 1 - core)
    d_xp, d_xm = at(zl, y, xp, zh, core), at(zl, y, xm, zh, core)
    d_yp, d_ym = at(zl, yp, x, zh, core), at(zl, ym, x, zh, core)
    d_zl = at(1 - zl, y, x, zh, core)
    d_zh = at(zl, y, x, 1 - zh, core)
    lin = row * 16 + col
    has_l, has_r = lin > 0, lin < 127
    left, right = jnp.maximum(lin - 1, 0), jnp.minimum(lin + 1, 127)
    d_left, d_right = (left // 16, left % 16), (right // 16, right % 16)

    own = pl.ds(HALF * LEAF, K * LEAF)
    c_panel = pltpu.make_async_copy(panel_hbm, pext.at[own], lsem.at[0])
    c_vt = pltpu.make_async_copy(vt_hbm, vt, lsem.at[1])
    c_ct = pltpu.make_async_copy(ct_hbm, ct, lsem.at[2])
    c_ut = pltpu.make_async_copy(
        ut_hbm.at[:, pl.ds(pl.multiple_of(col * (K * LEAF), K * LEAF), K * LEAF)], ut, lsem.at[3]
    )
    c_vt.start()
    c_panel.start()

    barrier = pltpu.get_barrier_semaphore()
    for dev in (d_core, d_xp, d_xm, d_yp, d_ym, d_zl, d_zh):
        pl.semaphore_signal(barrier, inc=1, device_id=dev, device_id_type=MESH)

    @pl.when(has_l)
    def _():
        pl.semaphore_signal(barrier, inc=1, device_id=d_left, device_id_type=MESH)

    @pl.when(has_r)
    def _():
        pl.semaphore_signal(barrier, inc=1, device_id=d_right, device_id_type=MESH)

    c_ct.start()
    c_ut.start()

    def near_copy(k):
        return pltpu.make_async_copy(near_hbm.at[k], nb.at[k], nsem.at[k])

    for k in list(range(4, 12)) + list(range(0, 4)) + list(range(12, 16)):
        near_copy(k).start()

    c_vt.wait()
    c_panel.wait()
    for k in range(K):
        v = mm(
            vt[:, k * LEAF:(k + 1) * LEAF], pext[(HALF + k) * LEAF:(HALF + k + 1) * LEAF, :]
        ).astype(BF16)
        call0[row * K + k] = v[:, :HN]
        call1[row * K + k] = v[:, HN:]

    pl.semaphore_wait(barrier, 7 + has_l.astype(jnp.int32) + has_r.astype(jnp.int32))

    def rc(m, src, dst, dev):
        return pltpu.make_async_remote_copy(
            src_ref=src, dst_ref=dst, send_sem=ssem.at[m], recv_sem=rsem.at[m],
            device_id=dev, device_id_type=MESH,
        )

    call = (call0, call1)

    def piece(q, m, slot, half, dev):
        ref = call[q].at[pl.ds(slot * K + half * 8, 8)]
        return rc(14 * q + m, ref, ref, dev)

    s_zp = (1 - zl) * 4 + y
    s_ym, s_yp = zl * 4 + ym, zl * 4 + yp
    sz_ym, sz_yp = (1 - zl) * 4 + ym, (1 - zl) * 4 + yp
    ga = [[
        piece(q, 0, row, 0, d_zl), piece(q, 1, row, 1, d_zl),
        piece(q, 2, row, 0, d_yp), piece(q, 3, row, 1, d_yp),
        piece(q, 4, row, 0, d_ym), piece(q, 5, row, 1, d_ym),
        piece(q, 6, s_zp, 0, d_yp), piece(q, 7, s_zp, 1, d_yp),
        piece(q, 8, s_zp, 0, d_ym), piece(q, 9, s_zp, 1, d_ym),
        piece(q, 10, s_ym, 0, d_yp), piece(q, 11, s_yp, 1, d_ym),
        piece(q, 12, sz_ym, 0, d_yp), piece(q, 13, sz_yp, 1, d_ym),
    ] for q in range(2)]

    def relay_own(q):
        ga[q][2].wait_recv()
        ga[q][10].start()
        ga[q][5].wait_recv()
        ga[q][11].start()

    def relay_z(q):
        ga[q][0].wait_recv()
        ga[q][6].start()
        ga[q][8].start()
        ga[q][1].wait_recv()
        ga[q][9].start()
        ga[q][7].start()

    def relay_far(q):
        ga[q][6].wait_recv()
        ga[q][12].start()
        ga[q][9].wait_recv()
        ga[q][13].start()

    def gathered(q):
        for m in (3, 4, 10, 11, 7, 8, 12, 13):
            ga[q][m].wait_recv()

    for m in (0, 2, 5, 1, 3, 4):
        ga[0][m].start()
    for m in (0, 1, 2, 5):
        ga[1][m].start()

    tail = pl.ds(K * LEAF, HALF * LEAF)
    head = pl.ds(HALF * LEAF, HALF * LEAF)
    lo = pl.ds(0, HALF * LEAF)
    hi = pl.ds((HALF + K) * LEAF, HALF * LEAF)
    h_right = rc(44, pext.at[tail], pext.at[lo], d_right)
    h_left = rc(45, pext.at[head], pext.at[hi], d_left)

    expand[...] = jnp.where(
        iota((R, 256), 1) % 16 == iota((R, 256), 0), 1.0, 0.0
    ).astype(BF16)
    c_ct.wait()
    keep = iota((SLOTS, 256), 0) % 16 == iota((SLOTS, 256), 1) // 16

    def l_rows(start, stop):
        def body(b, carry):
            for u in range(4):
                i = b * 4 + u
                v = mm_t(ct[i], expand[...])
                lmat[:, i] = jnp.where(keep, v, 0.0).astype(BF16).reshape(GROUPS, 16, 256)
            return carry
        lax.fori_loop(start // 4, stop // 4, body, 0)

    l_rows(0, 8)
    relay_own(0)
    relay_z(0)
    ga[1][3].start()
    ga[1][4].start()

    @pl.when(has_r)
    def _():
        h_right.start()

    @pl.when(has_l)
    def _():
        h_left.start()

    l_rows(8, 16)

    ra = iota((ROWCL, SLOTS), 0)
    kk, dz, pos, dc = ra % 16, 1 - (ra // 16) % 2, (ra // 32) % 4, 1 - ra // 128
    dx = jnp.where(pos == 0, 2, jnp.where(pos == 1, 1, jnp.where(pos == 2, 3, 0)))
    cluster = (((x + dx) % 4) * 4 + ((zh + dz) % 2) * 2 + (core + dc) % 2) * 16 + kk
    live = iota((ROWCL, SLOTS), 1) < cnt_ref[...]
    ohr[...] = jnp.where((cluster == rows_ref[...]) & live, 1.0, 0.0).astype(BF16)

    relay_own(1)
    relay_z(1)
    relay_far(0)

    def near_row(k):
        acc = mm(nb[k, 0], pext[pl.ds(pl.multiple_of(k * LEAF, LEAF), LEAF), :])
        for o in range(1, NEAR):
            acc += mm(nb[k, o], pext[pl.ds(pl.multiple_of((k + o) * LEAF, LEAF), LEAF), :])
        nearv[k] = acc

    def near_rows(start, stop):
        def body(k, carry):
            near_copy(k).wait()
            near_row(k)
            return carry
        lax.fori_loop(start, stop, body, 0)

    near_rows(4, 6)

    def couple(q):
        def body(b, carry):
            for u in range(4):
                g = b * 4 + u
                xs = [call[q][cols_ref[0, g * 16 + s]] for s in range(16)]
                t = mm(lmat[g].reshape(256, 256), jnp.concatenate(xs, axis=0))
                t = t.astype(BF16).reshape(8, 2, 16, HN)
                rows = pl.ds(pl.multiple_of(g * 16, 16), 16)
                tmat[:, rows, :HN] = t[:, 0]
                tmat[:, rows, HN:] = t[:, 1]
            return carry
        lax.fori_loop(0, GROUPS // 4, body, 0)

    def segment_sum(q):
        def body(b, carry):
            for u in range(4):
                i = b * 4 + u
                p = mm(ohr[...], tmat[i])
                for v in range(2):
                    lanes = slice(v * HN, (v + 1) * HN)
                    pp[q, :, :, 2 * i + v] = p[:128, lanes].astype(BF16).reshape(4, 2, 16, HN)
                    po[q, :, :, 2 * i + v] = p[128:, lanes].reshape(4, 2, 16, HN)
            return carry
        lax.fori_loop(0, 2, body, 0)

    def rcb(t, q, src, dst, dev):
        return rc(28 + 2 * t + q, src, dst, dev)

    qr = range(2)
    b0 = [rcb(0, q, pp.at[q], r0.at[q], d_core) for q in qr]
    b1p = [rcb(1, q, qs.at[q, 0, 0], r1.at[q, 0], d_xp) for q in qr]
    b1m = [rcb(2, q, qs.at[q, 0, 1], r1.at[q, 1], d_xm) for q in qr]
    b2p0 = [rcb(3, q, qs.at[q, 1, 1], r2.at[q, 0, 1], d_xp) for q in qr]
    b2m1 = [rcb(4, q, qs.at[q, 2, 0], r2.at[q, 1, 0], d_xm) for q in qr]
    b2p1 = [rcb(5, q, qs.at[q, 1, 0], r2.at[q, 0, 0], d_xp) for q in qr]
    b2m0 = [rcb(6, q, qs.at[q, 2, 1], r2.at[q, 1, 1], d_xm) for q in qr]
    bz = [rcb(7, q, zs.at[q], r3.at[q], d_zh) for q in qr]

    def fold(q, pos, dzi):
        return po[q, pos, dzi] + r0[q, pos, dzi].astype(F32)

    def x_first(q):
        b0[q].wait_recv()
        qs[q, 0, 0] = fold(q, 0, 0).astype(BF16)
        qs[q, 0, 1] = fold(q, 0, 1).astype(BF16)
        b1p[q].start()
        b1m[q].start()
        qs[q, 1, 1] = fold(q, 1, 1).astype(BF16)
        qs[q, 2, 0] = fold(q, 2, 0).astype(BF16)
        b2p0[q].start()
        b2m1[q].start()

    def x_second(q):
        b1p[q].wait_recv()
        qs[q, 1, 0] = (fold(q, 1, 0) + r1[q, 0].astype(F32)).astype(BF16)
        b2p1[q].start()
        b1m[q].wait_recv()
        qs[q, 2, 1] = (fold(q, 2, 1) + r1[q, 1].astype(F32)).astype(BF16)
        b2m0[q].start()

    def z_step(q):
        b2p1[q].wait_recv()
        b2m1[q].wait_recv()
        zs[q] = (
            fold(q, 3, 0) + r2[q, 0, 0].astype(F32) + r2[q, 1, 0].astype(F32)
        ).astype(BF16)
        bz[q].start()
        b2p0[q].wait_recv()
        b2m0[q].wait_recv()
        po[q, 3, 1] = fold(q, 3, 1) + r2[q, 0, 1].astype(F32) + r2[q, 1, 1].astype(F32)

    def finish(q):
        bz[q].wait_recv()
        c = (po[q, 3, 1] + r3[q].astype(F32)).astype(BF16).reshape(256, HN)
        cplk[:, q * HN:(q + 1) * HN] = mm(perm[...], c).astype(BF16)

    gathered(0)
    couple(0)
    relay_far(1)
    segment_sum(0)
    b0[0].start()
    near_rows(6, 8)
    x_first(0)
    gathered(1)
    couple(1)
    x_second(0)
    segment_sum(1)
    b0[1].start()

    perm[...] = jnp.where(
        (iota((256, 256), 1) // 16 == iota((256, 256), 0) % 16)
        & (iota((256, 256), 1) % 16 == iota((256, 256), 0) // 16), 1.0, 0.0
    ).astype(BF16)
    near_rows(8, 10)
    x_first(1)
    z_step(0)
    near_rows(10, 12)

    @pl.when(has_l)
    def _():
        h_right.wait_recv()

    @pl.when(jnp.logical_not(has_l))
    def _():
        pext[lo] = jnp.zeros((HALF * LEAF, N), BF16)

    @pl.when(has_r)
    def _():
        h_left.wait_recv()

    @pl.when(jnp.logical_not(has_r))
    def _():
        pext[hi] = jnp.zeros((HALF * LEAF, N), BF16)

    near_rows(0, 2)
    x_second(1)
    finish(0)
    c_ut.wait()
    utt[...] = ut[...].T
    near_rows(2, 4)
    near_rows(12, 14)
    z_step(1)
    near_rows(14, 16)
    finish(1)

    def o_body(b, carry):
        for u in range(4):
            k = b * 4 + u
            far = mm(
                utt[pl.ds(pl.multiple_of(k * LEAF, LEAF), LEAF), :],
                cplk[pl.ds(pl.multiple_of(k * R, R), R), :],
            )
            rows = pl.ds(pl.multiple_of(k * LEAF, LEAF), LEAF)
            out_ref[rows, :] = (nearv[k] + far).astype(BF16)
        return carry

    lax.fori_loop(0, K // 4, o_body, 0)

    for q in qr:
        for copy in ga[q]:
            copy.wait_send()
    for group in (b0, b1p, b1m, b2p0, b2m1, b2p1, b2m0, bz):
        for copy in group:
            copy.wait_send()

    @pl.when(has_r)
    def _():
        h_right.wait_send()

    @pl.when(has_l)
    def _():
        h_left.wait_send()


def hbm(v):
    return pltpu.with_memory_space_constraint(v, pltpu.HBM)


def on_device(panel, row_basis, col_basis, near_blocks, couplings, blk_rows, blk_cols, blk_count):
    any_ = pl.BlockSpec(memory_space=pltpu.HBM)
    vm = pl.BlockSpec(memory_space=pltpu.VMEM)
    sm = pl.BlockSpec(memory_space=pltpu.SMEM)
    scratch = [
        pltpu.VMEM(((K + 2 * HALF) * LEAF, N), BF16),
        pltpu.VMEM((R, K * LEAF), BF16),
        pltpu.VMEM((R, K * LEAF), BF16),
        pltpu.VMEM((K * LEAF, R), BF16),
        pltpu.VMEM((R, R, SLOTS), BF16),
        pltpu.VMEM((K, NEAR, LEAF, LEAF), BF16),
        pltpu.VMEM((128, R, HN), BF16),
        pltpu.VMEM((128, R, HN), BF16),
        pltpu.VMEM((R, 256), BF16),
        pltpu.VMEM((256, 256), BF16),
        pltpu.VMEM((GROUPS, R, 16, 256), BF16),
        pltpu.VMEM((R // 2, SLOTS, N), BF16),
        pltpu.VMEM((ROWCL, SLOTS), BF16),
        pltpu.VMEM((2, 4, 2, R, K, HN), BF16),
        pltpu.VMEM((2, 4, 2, R, K, HN), F32),
        pltpu.VMEM((2, 4, 2, R, K, HN), BF16),
        pltpu.VMEM((2, 3, 2, R, K, HN), BF16),
        pltpu.VMEM((2, 2, R, K, HN), BF16),
        pltpu.VMEM((2, 2, 2, R, K, HN), BF16),
        pltpu.VMEM((2, R, K, HN), BF16),
        pltpu.VMEM((2, R, K, HN), BF16),
        pltpu.VMEM((K * R, N), BF16),
        pltpu.VMEM((K, LEAF, N), F32),
        pltpu.SemaphoreType.DMA((4,)),
        pltpu.SemaphoreType.DMA((K,)),
        pltpu.SemaphoreType.DMA((46,)),
        pltpu.SemaphoreType.DMA((46,)),
    ]
    return pl.pallas_call(
        kernel,
        out_shape=pltpu.VMEM((K * LEAF, N), BF16),
        in_specs=[any_, any_, any_, any_, any_, vm, sm, vm],
        out_specs=vm,
        scratch_shapes=scratch,
        compiler_params=pltpu.CompilerParams(
            collective_id=0, has_side_effects=True, vmem_limit_bytes=64_800_000
        ),
    )(
        hbm(panel),
        hbm(row_basis.T),
        hbm(col_basis.T),
        hbm(near_blocks),
        hbm(couplings.reshape(SLOTS, R, R).transpose(1, 2, 0)),
        blk_rows.reshape(1, SLOTS),
        blk_cols.reshape(1, SLOTS),
        blk_count,
    )


def solution(mesh):
    placed = (
        P(("row", "col"), None),
        P("row", None),
        P(("row", "col"), None),
        P(("row", "col"), None, None, None),
        P("row", "col", None, None, None),
        P("row", "col", None),
        P("row", "col", None),
        P("row", "col"),
    )
    return jax.shard_map(
        on_device, mesh=mesh, in_specs=placed, out_specs=P(("row", "col"), None), check_vma=False
    )
```

```python
import jax
import jax.numpy as jnp
from jax import lax
from jax.experimental import pallas as pl
from jax.experimental.pallas import tpu as pltpu
from jax.sharding import PartitionSpec as P

MESH = pl.DeviceIdType.MESH
F32 = jnp.float32
BF16 = jnp.bfloat16

LEAF = 256
R = 16
N = 256
HN = N // 2
K = 16
HALF = 4
NEAR = 9
SLOTS = 512
GROUPS = SLOTS // 16
ROWCL = 256


def mm(a, b):
    return jnp.dot(a, b, preferred_element_type=F32)


def mm_t(a, b):
    return lax.dot_general(a, b, (((0,), (0,)), ((), ())), preferred_element_type=F32)


def iota(shape, dim):
    return lax.broadcasted_iota(jnp.int32, shape, dim)


def kernel(
    panel_hbm, ut_hbm, vt_hbm, near_hbm, ct_hbm, rows_hbm, cols_hbm, cnt_ref,
    out_ref,
    pext, vt, ut, utt, ct, nb, call0, call1, expand, perm, lmat, tmat, ohr,
    pp, po, r0, qs, r1, r2, zs, r3, cplk, nearv, rows_ref, cols_ref,
    lsem, nsem, ssem, rsem,
):
    row = lax.axis_index("row")
    col = lax.axis_index("col")
    zl, y = row // 4, row % 4
    x, zh, core = col // 4, (col // 2) % 2, col % 2

    def at(zl_, y_, x_, zh_, core_):
        return (zl_ * 4 + y_, x_ * 4 + zh_ * 2 + core_)

    yp, ym = (y + 1) % 4, (y + 3) % 4
    xp, xm = (x + 1) % 4, (x + 3) % 4
    d_core = at(zl, y, x, zh, 1 - core)
    d_xp, d_xm = at(zl, y, xp, zh, core), at(zl, y, xm, zh, core)
    d_yp, d_ym = at(zl, yp, x, zh, core), at(zl, ym, x, zh, core)
    d_zl = at(1 - zl, y, x, zh, core)
    d_zh = at(zl, y, x, 1 - zh, core)
    lin = row * 16 + col
    has_l, has_r = lin > 0, lin < 127
    left, right = jnp.maximum(lin - 1, 0), jnp.minimum(lin + 1, 127)
    d_left, d_right = (left // 16, left % 16), (right // 16, right % 16)

    own = pl.ds(HALF * LEAF, K * LEAF)
    c_panel = pltpu.make_async_copy(panel_hbm, pext.at[own], lsem.at[0])
    c_vt = pltpu.make_async_copy(vt_hbm, vt, lsem.at[1])
    c_ct = pltpu.make_async_copy(ct_hbm, ct, lsem.at[2])
    c_ut = pltpu.make_async_copy(
        ut_hbm.at[:, pl.ds(pl.multiple_of(col * (K * LEAF), K * LEAF), K * LEAF)], ut, lsem.at[3]
    )
    c_vt.start()
    c_panel.start()
    c_rows = pltpu.make_async_copy(rows_hbm, rows_ref, lsem.at[4])
    c_cols = pltpu.make_async_copy(cols_hbm, cols_ref, lsem.at[5])

    barrier = pltpu.get_barrier_semaphore()
    for dev in (d_core, d_xp, d_xm, d_yp, d_ym, d_zl, d_zh):
        pl.semaphore_signal(barrier, inc=1, device_id=dev, device_id_type=MESH)

    @pl.when(has_l)
    def _():
        pl.semaphore_signal(barrier, inc=1, device_id=d_left, device_id_type=MESH)

    @pl.when(has_r)
    def _():
        pl.semaphore_signal(barrier, inc=1, device_id=d_right, device_id_type=MESH)

    c_ct.start()
    c_rows.start()
    c_cols.start()
    c_ut.start()

    def near_copy(k):
        return pltpu.make_async_copy(near_hbm.at[k], nb.at[k], nsem.at[k])

    c_vt.wait()
    c_panel.wait()
    for k in range(K):
        v = mm(
            vt[:, k * LEAF:(k + 1) * LEAF], pext[(HALF + k) * LEAF:(HALF + k + 1) * LEAF, :]
        ).astype(BF16)
        call0[row * K + k] = v[:, :HN]
        call1[row * K + k] = v[:, HN:]

    pl.semaphore_wait(barrier, 7 + has_l.astype(jnp.int32) + has_r.astype(jnp.int32))

    def rc(m, src, dst, dev):
        return pltpu.make_async_remote_copy(
            src_ref=src, dst_ref=dst, send_sem=ssem.at[m], recv_sem=rsem.at[m],
            device_id=dev, device_id_type=MESH,
        )

    call = (call0, call1)

    def piece(q, m, slot, half, dev):
        ref = call[q].at[pl.ds(slot * K + half * 8, 8)]
        return rc(14 * q + m, ref, ref, dev)

    s_zp = (1 - zl) * 4 + y
    s_ym, s_yp = zl * 4 + ym, zl * 4 + yp
    sz_ym, sz_yp = (1 - zl) * 4 + ym, (1 - zl) * 4 + yp
    ga = [[
        piece(q, 0, row, 0, d_zl), piece(q, 1, row, 1, d_zl),
        piece(q, 2, row, 0, d_yp), piece(q, 3, row, 1, d_yp),
        piece(q, 4, row, 0, d_ym), piece(q, 5, row, 1, d_ym),
        piece(q, 6, s_zp, 0, d_yp), piece(q, 7, s_zp, 1, d_yp),
        piece(q, 8, s_zp, 0, d_ym), piece(q, 9, s_zp, 1, d_ym),
        piece(q, 10, s_ym, 0, d_yp), piece(q, 11, s_yp, 1, d_ym),
        piece(q, 12, sz_ym, 0, d_yp), piece(q, 13, sz_yp, 1, d_ym),
    ] for q in range(2)]

    def relay_own(q):
        ga[q][2].wait_recv()
        ga[q][10].start()
        ga[q][5].wait_recv()
        ga[q][11].start()

    def relay_z(q):
        ga[q][0].wait_recv()
        ga[q][6].start()
        ga[q][8].start()
        ga[q][1].wait_recv()
        ga[q][9].start()
        ga[q][7].start()

    def relay_far(q):
        ga[q][6].wait_recv()
        ga[q][12].start()
        ga[q][9].wait_recv()
        ga[q][13].start()

    def gathered(q):
        for m in (3, 4, 10, 11, 7, 8, 12, 13):
            ga[q][m].wait_recv()

    for m in (0, 2, 5, 1, 3, 4):
        ga[0][m].start()
    for m in (0, 1, 2, 5):
        ga[1][m].start()

    tail = pl.ds(K * LEAF, HALF * LEAF)
    head = pl.ds(HALF * LEAF, HALF * LEAF)
    lo = pl.ds(0, HALF * LEAF)
    hi = pl.ds((HALF + K) * LEAF, HALF * LEAF)
    h_right = rc(44, pext.at[tail], pext.at[lo], d_right)
    h_left = rc(45, pext.at[head], pext.at[hi], d_left)

    expand[...] = jnp.where(
        iota((R, 256), 1) % 16 == iota((R, 256), 0), 1.0, 0.0
    ).astype(BF16)
    c_ct.wait()
    c_rows.wait()
    c_cols.wait()
    for k in list(range(4, 12)) + list(range(0, 4)) + list(range(12, 16)):
        near_copy(k).start()
    keep = iota((SLOTS, 256), 0) % 16 == iota((SLOTS, 256), 1) // 16

    def l_rows(start, stop):
        def body(b, carry):
            for u in range(4):
                i = b * 4 + u
                v = mm_t(ct[i], expand[...])
                lmat[:, i] = jnp.where(keep, v, 0.0).astype(BF16).reshape(GROUPS, 16, 256)
            return carry
        lax.fori_loop(start // 4, stop // 4, body, 0)

    l_rows(0, 8)

    relay_own(0)
    relay_z(0)
    ga[1][3].start()
    ga[1][4].start()

    l_rows(8, 16)

    ra = iota((ROWCL, SLOTS), 0)
    kk, dz, pos, dc = ra % 16, 1 - (ra // 16) % 2, (ra // 32) % 4, 1 - ra // 128
    dx = jnp.where(pos == 0, 2, jnp.where(pos == 1, 1, jnp.where(pos == 2, 3, 0)))
    cluster = (((x + dx) % 4) * 4 + ((zh + dz) % 2) * 2 + (core + dc) % 2) * 16 + kk
    live = iota((ROWCL, SLOTS), 1) < cnt_ref[0, 0]
    ohr[...] = jnp.where((cluster == rows_ref[...]) & live, 1.0, 0.0).astype(BF16)

    relay_own(1)
    relay_z(1)
    relay_far(0)

    def near_row(k):
        acc = mm(nb[k, 0], pext[pl.ds(pl.multiple_of(k * LEAF, LEAF), LEAF), :])
        for o in range(1, NEAR):
            acc += mm(nb[k, o], pext[pl.ds(pl.multiple_of((k + o) * LEAF, LEAF), LEAF), :])
        nearv[k] = acc

    def near_rows(start, stop):
        def body(k, carry):
            near_copy(k).wait()
            near_row(k)
            return carry
        lax.fori_loop(start, stop, body, 0)

    near_rows(4, 6)

    def couple(q, start, stop):
        def body(b, carry):
            for u in range(4):
                g = b * 4 + u
                xs = [call[q][cols_ref[0, g * 16 + s]] for s in range(16)]
                t = mm(lmat[g].reshape(256, 256), jnp.concatenate(xs, axis=0))
                t = t.astype(BF16).reshape(8, 2, 16, HN)
                rows = pl.ds(pl.multiple_of(g * 16, 16), 16)
                tmat[:, rows, :HN] = t[:, 0]
                tmat[:, rows, HN:] = t[:, 1]
            return carry
        lax.fori_loop(start // 4, stop // 4, body, 0)

    def segment_sum(q):
        def body(b, carry):
            for u in range(4):
                i = b * 4 + u
                p = mm(ohr[...], tmat[i])
                for v in range(2):
                    lanes = slice(v * HN, (v + 1) * HN)
                    pp[q, :, :, 2 * i + v] = p[:128, lanes].astype(BF16).reshape(4, 2, 16, HN)
                    po[q, :, :, 2 * i + v] = p[128:, lanes].reshape(4, 2, 16, HN)
            return carry
        lax.fori_loop(0, 2, body, 0)

    def rcb(t, q, src, dst, dev):
        return rc(28 + 2 * t + q, src, dst, dev)

    qr = range(2)
    b0 = [rcb(0, q, pp.at[q], r0.at[q], d_core) for q in qr]
    b1p = [rcb(1, q, qs.at[q, 0, 0], r1.at[q, 0], d_xp) for q in qr]
    b1m = [rcb(2, q, qs.at[q, 0, 1], r1.at[q, 1], d_xm) for q in qr]
    b2p0 = [rcb(3, q, qs.at[q, 1, 1], r2.at[q, 0, 1], d_xp) for q in qr]
    b2m1 = [rcb(4, q, qs.at[q, 2, 0], r2.at[q, 1, 0], d_xm) for q in qr]
    b2p1 = [rcb(5, q, qs.at[q, 1, 0], r2.at[q, 0, 0], d_xp) for q in qr]
    b2m0 = [rcb(6, q, qs.at[q, 2, 1], r2.at[q, 1, 1], d_xm) for q in qr]
    bz = [rcb(7, q, zs.at[q], r3.at[q], d_zh) for q in qr]

    def fold(q, pos, dzi):
        return po[q, pos, dzi] + r0[q, pos, dzi].astype(F32)

    def x_first(q):
        b0[q].wait_recv()
        qs[q, 0, 0] = fold(q, 0, 0).astype(BF16)
        qs[q, 0, 1] = fold(q, 0, 1).astype(BF16)
        b1p[q].start()
        b1m[q].start()
        qs[q, 1, 1] = fold(q, 1, 1).astype(BF16)
        qs[q, 2, 0] = fold(q, 2, 0).astype(BF16)
        b2p0[q].start()
        b2m1[q].start()

    def x_second(q):
        b1p[q].wait_recv()
        qs[q, 1, 0] = (fold(q, 1, 0) + r1[q, 0].astype(F32)).astype(BF16)
        b2p1[q].start()
        b1m[q].wait_recv()
        qs[q, 2, 1] = (fold(q, 2, 1) + r1[q, 1].astype(F32)).astype(BF16)
        b2m0[q].start()

    def z_step(q):
        b2p1[q].wait_recv()
        b2m1[q].wait_recv()
        zs[q] = (
            fold(q, 3, 0) + r2[q, 0, 0].astype(F32) + r2[q, 1, 0].astype(F32)
        ).astype(BF16)
        bz[q].start()
        b2p0[q].wait_recv()
        b2m0[q].wait_recv()
        po[q, 3, 1] = fold(q, 3, 1) + r2[q, 0, 1].astype(F32) + r2[q, 1, 1].astype(F32)

    def finish(q):
        bz[q].wait_recv()
        c = (po[q, 3, 1] + r3[q].astype(F32)).astype(BF16).reshape(256, HN)
        cplk[:, q * HN:(q + 1) * HN] = mm(perm[...], c).astype(BF16)

    gathered(0)
    relay_far(1)

    @pl.when(has_r)
    def _():
        h_right.start()

    @pl.when(has_l)
    def _():
        h_left.start()

    couple(0, 0, GROUPS)
    segment_sum(0)
    b0[0].start()
    gathered(1)
    couple(1, 0, GROUPS // 2)
    x_first(0)
    couple(1, GROUPS // 2, GROUPS)
    segment_sum(1)
    b0[1].start()

    perm[...] = jnp.where(
        (iota((256, 256), 1) // 16 == iota((256, 256), 0) % 16)
        & (iota((256, 256), 1) % 16 == iota((256, 256), 0) // 16), 1.0, 0.0
    ).astype(BF16)
    near_rows(6, 7)
    x_second(0)
    x_first(1)
    near_rows(7, 12)
    z_step(0)

    @pl.when(has_l)
    def _():
        h_right.wait_recv()

    @pl.when(jnp.logical_not(has_l))
    def _():
        pext[lo] = jnp.zeros((HALF * LEAF, N), BF16)

    @pl.when(has_r)
    def _():
        h_left.wait_recv()

    @pl.when(jnp.logical_not(has_r))
    def _():
        pext[hi] = jnp.zeros((HALF * LEAF, N), BF16)

    x_second(1)
    c_ut.wait()
    utt[...] = ut[...].T
    near_rows(0, 4)
    near_rows(12, 14)
    finish(0)
    z_step(1)
    near_rows(14, 16)
    finish(1)

    def o_body(b, carry):
        for u in range(4):
            k = b * 4 + u
            far = mm(
                utt[pl.ds(pl.multiple_of(k * LEAF, LEAF), LEAF), :],
                cplk[pl.ds(pl.multiple_of(k * R, R), R), :],
            )
            rows = pl.ds(pl.multiple_of(k * LEAF, LEAF), LEAF)
            out_ref[rows, :] = (nearv[k] + far).astype(BF16)
        return carry

    lax.fori_loop(0, K // 4, o_body, 0)

    for q in qr:
        for copy in ga[q]:
            copy.wait_send()
    for group in (b0, b1p, b1m, b2p0, b2m1, b2p1, b2m0, bz):
        for copy in group:
            copy.wait_send()

    @pl.when(has_r)
    def _():
        h_right.wait_send()

    @pl.when(has_l)
    def _():
        h_left.wait_send()


def hbm(v):
    return pltpu.with_memory_space_constraint(v, pltpu.HBM)


def on_device(panel, row_basis, col_basis, near_blocks, couplings, blk_rows, blk_cols, blk_count):
    any_ = pl.BlockSpec(memory_space=pltpu.HBM)
    vm = pl.BlockSpec(memory_space=pltpu.VMEM)
    scratch = [
        pltpu.VMEM(((K + 2 * HALF) * LEAF, N), BF16),
        pltpu.VMEM((R, K * LEAF), BF16),
        pltpu.VMEM((R, K * LEAF), BF16),
        pltpu.VMEM((K * LEAF, R), BF16),
        pltpu.VMEM((R, R, SLOTS), BF16),
        pltpu.VMEM((K, NEAR, LEAF, LEAF), BF16),
        pltpu.VMEM((128, R, HN), BF16),
        pltpu.VMEM((128, R, HN), BF16),
        pltpu.VMEM((R, 256), BF16),
        pltpu.VMEM((256, 256), BF16),
        pltpu.VMEM((GROUPS, R, 16, 256), BF16),
        pltpu.VMEM((R // 2, SLOTS, N), BF16),
        pltpu.VMEM((ROWCL, SLOTS), BF16),
        pltpu.VMEM((2, 4, 2, R, K, HN), BF16),
        pltpu.VMEM((2, 4, 2, R, K, HN), F32),
        pltpu.VMEM((2, 4, 2, R, K, HN), BF16),
        pltpu.VMEM((2, 3, 2, R, K, HN), BF16),
        pltpu.VMEM((2, 2, R, K, HN), BF16),
        pltpu.VMEM((2, 2, 2, R, K, HN), BF16),
        pltpu.VMEM((2, R, K, HN), BF16),
        pltpu.VMEM((2, R, K, HN), BF16),
        pltpu.VMEM((K * R, N), BF16),
        pltpu.VMEM((K, LEAF, N), F32),
        pltpu.VMEM((1, SLOTS), jnp.int32),
        pltpu.SMEM((1, SLOTS), jnp.int32),
        pltpu.SemaphoreType.DMA((6,)),
        pltpu.SemaphoreType.DMA((K,)),
        pltpu.SemaphoreType.DMA((46,)),
        pltpu.SemaphoreType.DMA((46,)),
    ]
    return pl.pallas_call(
        kernel,
        out_shape=pltpu.VMEM((K * LEAF, N), BF16),
        in_specs=[any_] * 7 + [pl.BlockSpec(memory_space=pltpu.SMEM)],
        out_specs=vm,
        scratch_shapes=scratch,
        compiler_params=pltpu.CompilerParams(
            collective_id=0, has_side_effects=True, vmem_limit_bytes=64_800_000
        ),
    )(
        hbm(panel),
        hbm(row_basis.T),
        hbm(col_basis.T),
        hbm(near_blocks),
        hbm(couplings.reshape(SLOTS, R, R).transpose(1, 2, 0)),
        hbm(blk_rows.reshape(1, SLOTS)),
        hbm(blk_cols.reshape(1, SLOTS)),
        blk_count,
    )


def solution(mesh):
    placed = (
        P(("row", "col"), None),
        P("row", None),
        P(("row", "col"), None),
        P(("row", "col"), None, None, None),
        P("row", "col", None, None, None),
        P("row", "col", None),
        P("row", "col", None),
        P("row", "col"),
    )
    return jax.shard_map(
        on_device, mesh=mesh, in_specs=placed, out_specs=P(("row", "col"), None), check_vma=False
    )
```

```python
import jax
import jax.numpy as jnp
from jax import lax
from jax.experimental import pallas as pl
from jax.experimental.pallas import tpu as pltpu
from jax.sharding import PartitionSpec as P

MESH = pl.DeviceIdType.MESH
F32 = jnp.float32
BF16 = jnp.bfloat16

LEAF = 256
R = 16
N = 256
HN = N // 2
K = 16
HALF = 4
NEAR = 9
SLOTS = 512
GROUPS = SLOTS // 16
ROWCL = 256


def mm(a, b):
    return jnp.dot(a, b, preferred_element_type=F32)


def mm_t(a, b):
    return lax.dot_general(a, b, (((0,), (0,)), ((), ())), preferred_element_type=F32)


def iota(shape, dim):
    return lax.broadcasted_iota(jnp.int32, shape, dim)


def kernel(
    panel_hbm, ut_hbm, vt_hbm, near_hbm, ct_hbm, rows_hbm, cols_hbm, cnt_ref,
    out_ref,
    pext, vt, ut, utt, ct, nb, call0, call1, expand, perm, lmat, tmat, ohr,
    pp, po, r0, qs, r1, r2, zs, r3, cplk, nearv, rows_ref, cols_ref,
    lsem, nsem, ssem, rsem,
):
    row = lax.axis_index("row")
    col = lax.axis_index("col")
    zl, y = row // 4, row % 4
    x, zh, core = col // 4, (col // 2) % 2, col % 2

    def at(zl_, y_, x_, zh_, core_):
        return (zl_ * 4 + y_, x_ * 4 + zh_ * 2 + core_)

    yp, ym = (y + 1) % 4, (y + 3) % 4
    xp, xm = (x + 1) % 4, (x + 3) % 4
    d_core = at(zl, y, x, zh, 1 - core)
    d_xp, d_xm = at(zl, y, xp, zh, core), at(zl, y, xm, zh, core)
    d_yp, d_ym = at(zl, yp, x, zh, core), at(zl, ym, x, zh, core)
    d_zl = at(1 - zl, y, x, zh, core)
    d_y2 = at(zl, (y + 2) % 4, x, zh, core)
    d_zh = at(zl, y, x, 1 - zh, core)
    lin = row * 16 + col
    has_l, has_r = lin > 0, lin < 127
    left, right = jnp.maximum(lin - 1, 0), jnp.minimum(lin + 1, 127)
    d_left, d_right = (left // 16, left % 16), (right // 16, right % 16)

    own = pl.ds(HALF * LEAF, K * LEAF)
    c_panel = pltpu.make_async_copy(panel_hbm, pext.at[own], lsem.at[0])
    c_vt = pltpu.make_async_copy(vt_hbm, vt, lsem.at[1])
    c_ct = pltpu.make_async_copy(ct_hbm, ct, lsem.at[2])
    c_ut = pltpu.make_async_copy(
        ut_hbm.at[:, pl.ds(pl.multiple_of(col * (K * LEAF), K * LEAF), K * LEAF)], ut, lsem.at[3]
    )
    c_vt.start()
    c_panel.start()
    c_rows = pltpu.make_async_copy(rows_hbm, rows_ref, lsem.at[4])
    c_cols = pltpu.make_async_copy(cols_hbm, cols_ref, lsem.at[5])

    barrier = pltpu.get_barrier_semaphore()
    for dev in (d_core, d_xp, d_xm, d_yp, d_ym, d_y2, d_zl, d_zh):
        pl.semaphore_signal(barrier, inc=1, device_id=dev, device_id_type=MESH)

    @pl.when(has_l)
    def _():
        pl.semaphore_signal(barrier, inc=1, device_id=d_left, device_id_type=MESH)

    @pl.when(has_r)
    def _():
        pl.semaphore_signal(barrier, inc=1, device_id=d_right, device_id_type=MESH)

    c_ct.start()
    c_rows.start()
    c_cols.start()
    c_ut.start()

    def near_copy(k):
        return pltpu.make_async_copy(near_hbm.at[k], nb.at[k], nsem.at[k])

    c_vt.wait()
    c_panel.wait()
    for k in range(K):
        v = mm(
            vt[:, k * LEAF:(k + 1) * LEAF], pext[(HALF + k) * LEAF:(HALF + k + 1) * LEAF, :]
        ).astype(BF16)
        call0[row * K + k] = v[:, :HN]
        call1[row * K + k] = v[:, HN:]

    pl.semaphore_wait(barrier, 8 + has_l.astype(jnp.int32) + has_r.astype(jnp.int32))

    def rc(m, src, dst, dev):
        return pltpu.make_async_remote_copy(
            src_ref=src, dst_ref=dst, send_sem=ssem.at[m], recv_sem=rsem.at[m],
            device_id=dev, device_id_type=MESH,
        )

    call = (call0, call1)

    def piece(q, m, slot, half, dev):
        ref = call[q].at[pl.ds(slot * K + half * 8, 8)]
        return rc(14 * q + m, ref, ref, dev)

    s_zp = (1 - zl) * 4 + y
    s_ym, s_yp = zl * 4 + ym, zl * 4 + yp
    ga = [[
        piece(q, 0, row, 0, d_zl), piece(q, 1, row, 1, d_zl),
        piece(q, 2, row, 0, d_yp), piece(q, 3, row, 1, d_yp),
        piece(q, 4, row, 0, d_ym), piece(q, 5, row, 1, d_ym),
        piece(q, 6, s_zp, 0, d_yp), piece(q, 7, s_zp, 1, d_yp),
        piece(q, 8, s_zp, 0, d_ym), piece(q, 9, s_zp, 1, d_ym),
        piece(q, 10, s_ym, 0, d_yp), piece(q, 11, s_yp, 1, d_ym),
        piece(q, 12, s_zp, 0, d_y2), piece(q, 13, s_zp, 1, d_y2),
    ] for q in range(2)]

    def relay_own(q):
        ga[q][2].wait_recv()
        ga[q][10].start()
        ga[q][5].wait_recv()
        ga[q][11].start()

    def relay_z(q):
        ga[q][0].wait_recv()
        ga[q][12].start()
        ga[q][6].start()
        ga[q][8].start()
        ga[q][1].wait_recv()
        ga[q][13].start()
        ga[q][9].start()
        ga[q][7].start()

    def gathered(q):
        for m in (3, 4, 10, 11, 6, 9, 7, 8, 12, 13):
            ga[q][m].wait_recv()

    for m in (0, 2, 5, 1, 3, 4):
        ga[0][m].start()
    for m in (0, 1, 2, 5, 3, 4):
        ga[1][m].start()

    tail = pl.ds(K * LEAF, HALF * LEAF)
    head = pl.ds(HALF * LEAF, HALF * LEAF)
    lo = pl.ds(0, HALF * LEAF)
    hi = pl.ds((HALF + K) * LEAF, HALF * LEAF)
    h_right = rc(44, pext.at[tail], pext.at[lo], d_right)
    h_left = rc(45, pext.at[head], pext.at[hi], d_left)

    expand[...] = jnp.where(
        iota((R, 256), 1) % 16 == iota((R, 256), 0), 1.0, 0.0
    ).astype(BF16)
    c_ct.wait()
    c_rows.wait()
    c_cols.wait()
    for k in list(range(4, 12)) + list(range(0, 4)) + list(range(12, 16)):
        near_copy(k).start()
    keep = iota((SLOTS, 256), 0) % 16 == iota((SLOTS, 256), 1) // 16

    def l_rows(start, stop):
        def body(b, carry):
            for u in range(4):
                i = b * 4 + u
                v = mm_t(ct[i], expand[...])
                lmat[:, i] = jnp.where(keep, v, 0.0).astype(BF16).reshape(GROUPS, 16, 256)
            return carry
        lax.fori_loop(start // 4, stop // 4, body, 0)

    l_rows(0, 8)

    relay_own(0)
    relay_z(0)

    l_rows(8, 16)

    ra = iota((ROWCL, SLOTS), 0)
    kk, dz, pos, dc = ra % 16, 1 - (ra // 16) % 2, (ra // 32) % 4, 1 - ra // 128
    dx = jnp.where(pos == 0, 2, jnp.where(pos == 1, 1, jnp.where(pos == 2, 3, 0)))
    cluster = (((x + dx) % 4) * 4 + ((zh + dz) % 2) * 2 + (core + dc) % 2) * 16 + kk
    live = iota((ROWCL, SLOTS), 1) < cnt_ref[0, 0]
    ohr[...] = jnp.where((cluster == rows_ref[...]) & live, 1.0, 0.0).astype(BF16)

    relay_own(1)
    relay_z(1)

    def near_row(k):
        acc = mm(nb[k, 0], pext[pl.ds(pl.multiple_of(k * LEAF, LEAF), LEAF), :])
        for o in range(1, NEAR):
            acc += mm(nb[k, o], pext[pl.ds(pl.multiple_of((k + o) * LEAF, LEAF), LEAF), :])
        nearv[k] = acc

    def near_rows(start, stop):
        def body(k, carry):
            near_copy(k).wait()
            near_row(k)
            return carry
        lax.fori_loop(start, stop, body, 0)

    near_rows(4, 6)

    def couple(q, start, stop):
        def body(b, carry):
            for u in range(4):
                g = b * 4 + u
                xs = [call[q][cols_ref[0, g * 16 + s]] for s in range(16)]
                t = mm(lmat[g].reshape(256, 256), jnp.concatenate(xs, axis=0))
                t = t.astype(BF16).reshape(8, 2, 16, HN)
                rows = pl.ds(pl.multiple_of(g * 16, 16), 16)
                tmat[:, rows, :HN] = t[:, 0]
                tmat[:, rows, HN:] = t[:, 1]
            return carry
        lax.fori_loop(start // 4, stop // 4, body, 0)

    def segment_sum(q):
        def body(b, carry):
            for u in range(4):
                i = b * 4 + u
                p = mm(ohr[...], tmat[i])
                for v in range(2):
                    lanes = slice(v * HN, (v + 1) * HN)
                    pp[q, :, :, 2 * i + v] = p[:128, lanes].astype(BF16).reshape(4, 2, 16, HN)
                    po[q, :, :, 2 * i + v] = p[128:, lanes].reshape(4, 2, 16, HN)
            return carry
        lax.fori_loop(0, 2, body, 0)

    def rcb(t, q, src, dst, dev):
        return rc(28 + 2 * t + q, src, dst, dev)

    qr = range(2)
    b0 = [[rc(46 + 4 * q + p, pp.at[q, p], r0.at[q, p], d_core) for p in range(4)] for q in qr]

    def core_send(q):
        for copy in b0[q]:
            copy.start()

    b1p = [rcb(1, q, qs.at[q, 0, 0], r1.at[q, 0], d_xp) for q in qr]
    b1m = [rcb(2, q, qs.at[q, 0, 1], r1.at[q, 1], d_xm) for q in qr]
    b2p0 = [rcb(3, q, qs.at[q, 1, 1], r2.at[q, 0, 1], d_xp) for q in qr]
    b2m1 = [rcb(4, q, qs.at[q, 2, 0], r2.at[q, 1, 0], d_xm) for q in qr]
    b2p1 = [rcb(5, q, qs.at[q, 1, 0], r2.at[q, 0, 0], d_xp) for q in qr]
    b2m0 = [rcb(6, q, qs.at[q, 2, 1], r2.at[q, 1, 1], d_xm) for q in qr]
    bz = [rcb(7, q, zs.at[q], r3.at[q], d_zh) for q in qr]

    def fold(q, pos, dzi):
        return po[q, pos, dzi] + r0[q, pos, dzi].astype(F32)

    def x_first(q):
        b0[q][0].wait_recv()
        qs[q, 0, 0] = fold(q, 0, 0).astype(BF16)
        qs[q, 0, 1] = fold(q, 0, 1).astype(BF16)
        b1p[q].start()
        b1m[q].start()
        b0[q][1].wait_recv()
        b0[q][2].wait_recv()
        qs[q, 1, 1] = fold(q, 1, 1).astype(BF16)
        qs[q, 2, 0] = fold(q, 2, 0).astype(BF16)
        b2p0[q].start()
        b2m1[q].start()

    def x_second(q):
        b1p[q].wait_recv()
        qs[q, 1, 0] = (fold(q, 1, 0) + r1[q, 0].astype(F32)).astype(BF16)
        b2p1[q].start()
        b1m[q].wait_recv()
        qs[q, 2, 1] = (fold(q, 2, 1) + r1[q, 1].astype(F32)).astype(BF16)
        b2m0[q].start()

    def z_step(q):
        b0[q][3].wait_recv()
        b2p1[q].wait_recv()
        b2m1[q].wait_recv()
        zs[q] = (
            fold(q, 3, 0) + r2[q, 0, 0].astype(F32) + r2[q, 1, 0].astype(F32)
        ).astype(BF16)
        bz[q].start()
        b2p0[q].wait_recv()
        b2m0[q].wait_recv()
        po[q, 3, 1] = fold(q, 3, 1) + r2[q, 0, 1].astype(F32) + r2[q, 1, 1].astype(F32)

    def finish(q):
        bz[q].wait_recv()
        c = (po[q, 3, 1] + r3[q].astype(F32)).astype(BF16).reshape(256, HN)
        cplk[:, q * HN:(q + 1) * HN] = mm(perm[...], c).astype(BF16)

    gathered(0)

    @pl.when(has_r)
    def _():
        h_right.start()

    @pl.when(has_l)
    def _():
        h_left.start()

    couple(0, 0, GROUPS)
    segment_sum(0)
    core_send(0)
    gathered(1)
    couple(1, 0, GROUPS // 2)
    x_first(0)
    couple(1, GROUPS // 2, GROUPS)
    segment_sum(1)
    core_send(1)

    perm[...] = jnp.where(
        (iota((256, 256), 1) // 16 == iota((256, 256), 0) % 16)
        & (iota((256, 256), 1) % 16 == iota((256, 256), 0) // 16), 1.0, 0.0
    ).astype(BF16)
    near_rows(6, 7)
    x_second(0)
    x_first(1)
    near_rows(7, 12)
    z_step(0)

    @pl.when(has_l)
    def _():
        h_right.wait_recv()

    @pl.when(jnp.logical_not(has_l))
    def _():
        pext[lo] = jnp.zeros((HALF * LEAF, N), BF16)

    @pl.when(has_r)
    def _():
        h_left.wait_recv()

    @pl.when(jnp.logical_not(has_r))
    def _():
        pext[hi] = jnp.zeros((HALF * LEAF, N), BF16)

    x_second(1)
    c_ut.wait()
    utt[...] = ut[...].T
    near_rows(0, 4)
    near_rows(12, 14)
    finish(0)
    z_step(1)
    near_rows(14, 16)
    finish(1)

    def o_body(b, carry):
        for u in range(4):
            k = b * 4 + u
            far = mm(
                utt[pl.ds(pl.multiple_of(k * LEAF, LEAF), LEAF), :],
                cplk[pl.ds(pl.multiple_of(k * R, R), R), :],
            )
            rows = pl.ds(pl.multiple_of(k * LEAF, LEAF), LEAF)
            out_ref[rows, :] = (nearv[k] + far).astype(BF16)
        return carry

    lax.fori_loop(0, K // 4, o_body, 0)

    for q in qr:
        for copy in ga[q]:
            copy.wait_send()
    for group in (b0[0], b0[1], b1p, b1m, b2p0, b2m1, b2p1, b2m0, bz):
        for copy in group:
            copy.wait_send()

    @pl.when(has_r)
    def _():
        h_right.wait_send()

    @pl.when(has_l)
    def _():
        h_left.wait_send()


def hbm(v):
    return pltpu.with_memory_space_constraint(v, pltpu.HBM)


def on_device(panel, row_basis, col_basis, near_blocks, couplings, blk_rows, blk_cols, blk_count):
    any_ = pl.BlockSpec(memory_space=pltpu.HBM)
    vm = pl.BlockSpec(memory_space=pltpu.VMEM)
    scratch = [
        pltpu.VMEM(((K + 2 * HALF) * LEAF, N), BF16),
        pltpu.VMEM((R, K * LEAF), BF16),
        pltpu.VMEM((R, K * LEAF), BF16),
        pltpu.VMEM((K * LEAF, R), BF16),
        pltpu.VMEM((R, R, SLOTS), BF16),
        pltpu.VMEM((K, NEAR, LEAF, LEAF), BF16),
        pltpu.VMEM((128, R, HN), BF16),
        pltpu.VMEM((128, R, HN), BF16),
        pltpu.VMEM((R, 256), BF16),
        pltpu.VMEM((256, 256), BF16),
        pltpu.VMEM((GROUPS, R, 16, 256), BF16),
        pltpu.VMEM((R // 2, SLOTS, N), BF16),
        pltpu.VMEM((ROWCL, SLOTS), BF16),
        pltpu.VMEM((2, 4, 2, R, K, HN), BF16),
        pltpu.VMEM((2, 4, 2, R, K, HN), F32),
        pltpu.VMEM((2, 4, 2, R, K, HN), BF16),
        pltpu.VMEM((2, 3, 2, R, K, HN), BF16),
        pltpu.VMEM((2, 2, R, K, HN), BF16),
        pltpu.VMEM((2, 2, 2, R, K, HN), BF16),
        pltpu.VMEM((2, R, K, HN), BF16),
        pltpu.VMEM((2, R, K, HN), BF16),
        pltpu.VMEM((K * R, N), BF16),
        pltpu.VMEM((K, LEAF, N), F32),
        pltpu.VMEM((1, SLOTS), jnp.int32),
        pltpu.SMEM((1, SLOTS), jnp.int32),
        pltpu.SemaphoreType.DMA((6,)),
        pltpu.SemaphoreType.DMA((K,)),
        pltpu.SemaphoreType.DMA((54,)),
        pltpu.SemaphoreType.DMA((54,)),
    ]
    return pl.pallas_call(
        kernel,
        out_shape=pltpu.VMEM((K * LEAF, N), BF16),
        in_specs=[any_] * 7 + [pl.BlockSpec(memory_space=pltpu.SMEM)],
        out_specs=vm,
        scratch_shapes=scratch,
        compiler_params=pltpu.CompilerParams(
            collective_id=0, has_side_effects=True, vmem_limit_bytes=64_800_000
        ),
    )(
        hbm(panel),
        hbm(row_basis.T),
        hbm(col_basis.T),
        hbm(near_blocks),
        hbm(couplings.reshape(SLOTS, R, R).transpose(1, 2, 0)),
        hbm(blk_rows.reshape(1, SLOTS)),
        hbm(blk_cols.reshape(1, SLOTS)),
        blk_count,
    )


def solution(mesh):
    placed = (
        P(("row", "col"), None),
        P("row", None),
        P(("row", "col"), None),
        P(("row", "col"), None, None, None),
        P("row", "col", None, None, None),
        P("row", "col", None),
        P("row", "col", None),
        P("row", "col"),
    )
    return jax.shard_map(
        on_device, mesh=mesh, in_specs=placed, out_specs=P(("row", "col"), None), check_vma=False
    )
```
